32 devices in a mesh: seq: 8 (over z, y), head: 4 (over x, core).
Axes of the slice: x: 2, y: 2, z: 4, core: 2. Of those that a mesh axis runs over, the one named last changes fastest.
Arguments:
- hidden_states: bfloat16 [8, 512, 3584], P(None, 'seq', 'head'), may hold values from -6 to 6
- boundary: int32 [8, 64], replicated, may hold values from 0 to 511, as said below
- valid: int32 [8, 64], replicated, may hold values from 0 to 1, as said below
- pairs: int32 [8, 2], replicated, may hold values from 0 to 7, as said below
- w_first: bfloat16 [3584, 4096], P('seq', 'head'), may hold values from -0.09375 to 0.09375
- b_first: float32 [4096], P('head'), may hold values from -3 to 3
- w_second: float32 [4096], P('head'), may hold values from -0.09375 to 0.09375
Outputs:
- step_reward: float32 [8, 64], replicated
- trace_score: float32 [8], replicated
- margin: float32 [8], replicated
The draws below stay inside these ranges and needn't reach their ends.
Inputs may be any that keep to these rules, and one draw needn't show every extreme that they name: Within a trace the 64 boundary positions are distinct and increasing. In each trace the ones come first; every trace has 16 to 64 valid steps. `pairs`: the two traces of a pair differ.
All inputs are finite; a program needn't handle non-finite values.
Results may differ from the reference program's by a relative error of at most 0.0003.
Values may be sent and summed in bfloat16 or wider, within the bound.
A program may use at most 64 MiB of HBM per device.

```python
import jax
import jax.numpy as jnp

D = 3584
HID = 4096
STEPS = 64
TRACES = 8
SEQLEN = 512
PAIRS = 8


def count_steps(key):
    return jax.random.randint(jax.random.fold_in(key, 11), (TRACES,), 16, STEPS + 1)


def draw_boundary(key, part):
    keys = jax.random.split(jax.random.fold_in(key, 23), TRACES)

    def one_trace(single):
        chosen = jax.random.permutation(single, SEQLEN)[:STEPS]
        return jnp.sort(chosen)
    return jax.vmap(one_trace)(keys).astype(jnp.int32)


def draw_valid(key, part):
    counts = count_steps(key)
    slots = jnp.arange(STEPS)[None, :]
    return (slots < counts[:, None]).astype(jnp.int32)


def draw_pairs(key, part):
    first = jax.random.randint(jax.random.fold_in(key, 31), (PAIRS,), 0, TRACES)
    offset = jax.random.randint(jax.random.fold_in(key, 37), (PAIRS,), 1, TRACES)
    second = (first + offset) % TRACES
    return jnp.stack([first, second], axis=1).astype(jnp.int32)


def block_scale(rng, dims, shards, smallest, top_value):
    def one(position, parts):
        draws = jax.random.uniform(jax.random.fold_in(jax.random.fold_in(rng, 6), position), (parts,), jnp.float32, smallest / len(shards), top_value / len(shards))
        return jnp.repeat(jnp.exp(draws), dims[position] // parts).reshape((-1,) + (1,) * (len(dims) - position - 1))

    level = one(*shards[0])
    for cut in shards[1:]:
        level = level * one(*cut)
    return level


def noise(key, extent, spread, most, pieces=(), kind=jnp.bfloat16):
    loudness = block_scale(key, extent, pieces, -0.22, 0.18) if pieces else 1.0
    entries = jax.random.normal(key, extent, jnp.float32) * spread * loudness
    return jnp.minimum(jnp.maximum(entries, -most), most).astype(kind)


def setup_inputs(seed: int = 0) -> dict:
    arg_keys = jax.random.split(jax.random.key(seed), 8)
    hidden_states = noise(arg_keys[0], (TRACES, SEQLEN, D), 1.0, 6.0, ((1, 8), (2, 4)))
    boundary = draw_boundary(jax.random.fold_in(arg_keys[7], 71), 0)
    valid = draw_valid(jax.random.fold_in(arg_keys[7], 71), 0)
    pairs = draw_pairs(jax.random.fold_in(arg_keys[7], 71), 0)
    w_first = noise(arg_keys[4], (D, HID), D ** -0.5, 0.09375, ((0, 8), (1, 4)))
    b_first = noise(arg_keys[5], (HID,), 0.5, 3.0, ((0, 4),), jnp.float32)
    w_second = noise(arg_keys[6], (HID,), HID ** -0.5, 0.09375, ((0, 4),), jnp.float32)
    return dict(hidden_states=hidden_states, boundary=boundary, valid=valid, pairs=pairs, w_first=w_first, b_first=b_first, w_second=w_second)


def reference(hidden_states, boundary, valid, pairs, w_first, b_first, w_second):
    picked = jnp.take_along_axis(hidden_states, boundary[:, :, None].astype(jnp.int32), axis=1)
    rows = picked.reshape(TRACES * STEPS, D)
    pre = jnp.dot(rows, w_first, preferred_element_type=jnp.float32) + b_first
    logit = jnp.sum(jnp.maximum(pre, 0.0) * w_second, axis=-1).reshape(TRACES, STEPS)
    live = valid == 1
    step_reward = jnp.where(live, logit, jnp.float32(0.0))
    trace_score = jnp.min(jnp.where(live, logit, jnp.float32(1e30)), axis=1)
    margin = trace_score[pairs[:, 0]] - trace_score[pairs[:, 1]]
    return step_reward, trace_score, margin
```

```python
import functools

import jax
import jax.numpy as jnp
from jax import lax
from jax.experimental import pallas as pl
from jax.experimental.pallas import tpu as pltpu
from jax.sharding import PartitionSpec as P

MESH = pl.DeviceIdType.MESH
SPAN = 128
HUB_FIRST = 0
EARLY = 1
W_MEMBER = (-8, -6, -4, -1)
W_OUTER = (-8, 7, 7, 7)
W_MIDDLE = (-8, -6, -4, -1)
PARTS = 1
AHEAD = 1
LAG_Y = 8
LAG_Z = 16


def schedule(blocks, chunks):
    order = [(k, c) for k in range(blocks) for c in range(chunks)]
    left = {k: chunks for k in range(blocks)}
    ops, pending, got = [], [], 0
    for i in range(len(order) + LAG_Y):
        if i < len(order):
            k, c = order[i]
            while got < min(blocks, k + 1 + AHEAD):
                ops.append((0, got, 0))
                got += 1
            if c == 0:
                ops.append((1, k, 0))
            ops.append((2, k, c))
        if i >= LAG_Y:
            k, c = order[i - LAG_Y]
            ops.append((3, k, c))
            left[k] -= 1
            if left[k] == 0:
                pending.append((i + LAG_Z, k))
        while pending and pending[0][0] <= i:
            ops.append((4, pending.pop(0)[1], 0))
    return ops + [(4, k, 0) for _, k in pending]


def score_rows(rows, w_first, b_first, w_second):
    pre = jnp.dot(
        rows, lax.all_gather(w_first, "seq", axis=0, tiled=True), preferred_element_type=jnp.float32
    )
    return jnp.sum(jnp.maximum(pre + b_first, 0.0) * w_second, axis=-1)


def per_device(hidden_states, boundary, valid, pairs, w_first, b_first, w_second):
    traces, tok_dev, quarter = hidden_states.shape
    offset = lax.axis_index("seq") * tok_dev
    positions = offset + jnp.arange(tok_dev, dtype=jnp.int32)
    hits = boundary[:, :, None] == positions[None, None, :]
    whole = lax.all_gather(hidden_states, "head", axis=2, tiled=True)
    token_logit = score_rows(
        whole.reshape(traces * tok_dev, whole.shape[2]), w_first, b_first, w_second
    )
    token_logit = token_logit.reshape(traces, tok_dev)
    partial_logit = jnp.sum(jnp.where(hits, token_logit[:, None, :], 0.0), axis=2)
    logit = lax.psum(partial_logit, ("seq", "head"))
    live = valid == 1
    step_reward = jnp.where(live, logit, jnp.float32(0.0))
    trace_score = jnp.min(jnp.where(live, logit, jnp.float32(1e30)), axis=1)
    trace_ids = jnp.arange(traces, dtype=jnp.int32)[None, :]
    winner = jnp.sum(jnp.where(pairs[:, 0:1] == trace_ids, trace_score[None, :], 0.0), axis=1)
    loser = jnp.sum(jnp.where(pairs[:, 1:2] == trace_ids, trace_score[None, :], 0.0), axis=1)
    return (step_reward, trace_score, winner - loser)


def kernel(
    n_seq, n_head, hid_hbm, bnd, valid, pairs, w_hbm, b, w2, result,
    hid, xo, xin, xup, xdn, xq, xl, wown, wall,
    ysend, yrecv, zsend, zrecv, kept, fsend, frecv, far,
    s_hid, s_win, s_x1, r_x1, s_w, r_w, s_x2, r_up, r_dn, s_x3, r_x3,
    s_y, r_y, s_z, r_z, s_f, r_f,
):
    traces, toks, feats = hid.shape
    blocks, block, _ = xin.shape
    steps = bnd.shape[1]
    planes = n_seq // 2
    depth = w_hbm.shape[0]
    cols = w_hbm.shape[1] // 2
    chunks, _, span = wown.shape
    groups = traces // 2
    s = lax.axis_index("seq")
    h = lax.axis_index("head")
    z = s // 2
    y = s % 2
    other = 1 - y
    odd = z % 2
    high = z // 2
    par = h % 2
    lanes = lax.broadcasted_iota(jnp.int32, (block, feats), 1)

    def fetch_w(c, mine):
        first = pl.multiple_of((odd if mine else 1 - odd) * cols + c * span, span)
        rows = pl.ds(pl.multiple_of(odd * depth, depth), depth)
        return pltpu.make_async_copy(
            w_hbm.at[:, pl.ds(first, span)],
            wall.at[c, rows, :] if mine else wown.at[c],
            s_win.at[c, 1 if mine else 0],
        )

    def trace_of(k):
        return (k % 2) * groups + k // 2

    def fetch_hid(k):
        t = trace_of(k)
        return pltpu.make_async_copy(hid_hbm.at[t], hid.at[t], s_hid.at[t])

    for k in range(blocks):
        fetch_hid(k).start()
        if k % 2 == 1 and k // 2 < chunks:
            fetch_w(k // 2, False).start()

    def remote(src, dst, send, recv, to_s, to_h):
        return pltpu.make_async_remote_copy(
            src_ref=src, dst_ref=dst, send_sem=send, recv_sem=recv,
            device_id=(to_s, to_h), device_id_type=MESH,
        )

    across = s + 1 - 2 * y
    h_core = h + 1 - 2 * par
    h_x = lax.rem(h + 2, n_head)
    s_near = s + 2 - 4 * odd
    s_far = lax.rem(s + n_seq // 2, n_seq)
    is_end = (z == 0) | (z == planes - 1)
    middle = jnp.logical_not(is_end)
    member = (h // 2) == high
    hub = member & middle

    barrier = pltpu.get_barrier_semaphore()

    def greet(to_s, to_h):
        pl.semaphore_signal(barrier, inc=1, device_id=(to_s, to_h), device_id_type=MESH)

    greet(across, h)
    greet(s, h_core)
    greet(s, h_x)

    @pl.when(z > 0)
    def _():
        greet(s - 2, h)

    @pl.when(z < planes - 1)
    def _():
        greet(s + 2, h)

    def turn(rows):
        return jnp.concatenate([rows[:, feats // 2 :], rows[:, : feats // 2]], axis=1)

    def fold(low, high_rows):
        return (
            jnp.where(lanes < feats // 2, low, turn(high_rows)),
            jnp.where(lanes < feats // 2, turn(low), high_rows),
        )

    def pick(k):
        t = trace_of(k)
        fetch_hid(k).wait()
        pos = lax.broadcasted_iota(jnp.int32, (toks, steps), 0) + s * toks
        hot = jnp.where(bnd[pl.ds(t, 1), :] == pos, 1.0, 0.0).astype(jnp.bfloat16)
        got = lax.dot_general(
            hot, hid[t], (((0,), (0,)), ((), ())), preferred_element_type=jnp.float32
        )
        pair = fold(got[:block], got[block:])
        for half in range(2):
            xo[half, k] = pair[half].astype(jnp.bfloat16)

    size = block // PARTS
    pieces = blocks * PARTS

    def rows_of(n):
        return pl.ds((n % PARTS) * size, size)

    def copy_x1(n):
        k, rows = n // PARTS, rows_of(n)
        return remote(
            xo.at[other, k, rows], xin.at[k, rows], s_x1.at[n], r_x1.at[n], across, h
        )

    def copy_w(c):
        rows = pl.ds(pl.multiple_of(odd * depth, depth), depth)
        return remote(wown.at[c], wall.at[c, rows, :], s_w.at[c], r_w.at[c], s_near, h)

    for k in range(EARLY):
        pick(k)
    pl.semaphore_wait(
        barrier, 3 + jnp.where(z > 0, 1, 0) + jnp.where(z < planes - 1, 1, 0)
    )
    def send_w(k):
        for c in range(chunks):
            for plan, who in (
                (W_MEMBER, member & is_end),
                (W_OUTER, jnp.logical_not(member) & is_end),
                (W_MIDDLE, middle),
            ):
                if plan[c] == k:

                    @pl.when(who)
                    def _():
                        fetch_w(c, False).wait()
                        copy_w(c).start()

    for k in range(blocks):
        if k >= EARLY:
            pick(k)
        for p in range(PARTS):
            copy_x1(k * PARTS + p).start()
        send_w(k - blocks)
    for c in range(chunks):
        fetch_w(c, True).start()

    @pl.when(middle)
    def _():
        pl.semaphore_signal(far, inc=1, device_id=(s - 2, h), device_id_type=MESH)
        pl.semaphore_signal(far, inc=1, device_id=(s + 2, h), device_id_type=MESH)

    def copy_up(n):
        k, rows = n // PARTS, rows_of(n)
        to_s = jnp.where(member, s_near, jnp.where(h >= n_head // 2, s + 2, s - 2))
        return remote(
            xo.at[y, k, rows], xup.at[k, rows], s_x2.at[n], r_up.at[n],
            lax.rem(to_s + n_seq, n_seq), h,
        )

    def copy_dn(n):
        k, rows = n // PARTS, rows_of(n)
        return remote(xo.at[y, k, rows], xdn.at[k, rows], s_x2.at[n], r_dn.at[n], s_near, h)

    def copy_x3(q, n, way):
        k, rows = n // PARTS, rows_of(n)
        to_h = h_x if way else h_core
        return remote(
            xq.at[q, k, rows], xq.at[q, k, rows], s_x3.at[way * pieces + n],
            r_x3.at[q * pieces + n], s, to_h,
        )

    def relay(n):
        k, rows = n // PARTS, rows_of(n)
        copy_x1(n).wait_recv()
        xo[y, k, rows] = xo[y, k, rows] + xin[k, rows]

        @pl.when(middle)
        def _():
            copy_up(n).wait_recv()
            xo[y, k, rows] = xo[y, k, rows] + xup[k, rows]

        @pl.when(member)
        def _():
            copy_dn(n).start()

        @pl.when(jnp.logical_not(member))
        def _():
            copy_up(n).start()

    def gather(n):
        k, rows = n // PARTS, rows_of(n)
        copy_x1(n).wait_recv()
        copy_up(n).wait_recv()
        xo[y, k, rows] = (xo[y, k, rows] + xin[k, rows]) + xup[k, rows]
        copy_up(n).start()
        copy_dn(n).wait_recv()
        xq[par, k, rows] = xo[y, k, rows] + xdn[k, rows]
        copy_x3(par, n, 1).start()
        copy_x3(par, n, 0).start()

    def collect(n):
        k, rows = n // PARTS, rows_of(n)
        if k >= HUB_FIRST:

            @pl.when(hub)
            def _():
                gather(n)

        @pl.when(member & is_end)
        def _():
            copy_up(n).wait_recv()
            xq[par, k, rows] = xo[y, k, rows] + xup[k, rows]
            copy_x3(par, n, 1).start()

        @pl.when(jnp.logical_not(member))
        def _():
            copy_x3(par, n, 1).wait_recv()

        @pl.when(jnp.logical_not(hub))
        def _():
            copy_x3(par, n, 0).start()

    def ready(k):
        for p in range(PARTS):
            copy_x3(1 - par, k * PARTS + p, 0).wait_recv()
        low = xq[0, k].astype(jnp.float32)
        top = xq[1, k].astype(jnp.float32)
        pair = fold(low, top)
        xl[k, :block] = pair[0].astype(jnp.bfloat16)
        xl[k, block:] = pair[1].astype(jnp.bfloat16)

    @pl.when(jnp.logical_not(hub))
    def _():
        for k in range(blocks):
            for p in range(PARTS):
                relay(k * PARTS + p)
            send_w(k)

    @pl.when(hub)
    def _():
        for n in range(HUB_FIRST * PARTS):
            gather(n)

    def copy_y(t):
        return remote(ysend.at[t], yrecv.at[t], s_y.at[t], r_y.at[t], across, h)

    def copy_z(t):
        return remote(zsend.at[t], zrecv.at[t], s_z.at[t], r_z.at[t], s_far, h)

    spots = lax.broadcasted_iota(jnp.int32, (steps, 128), 1)
    fsend[...] = jnp.zeros_like(fsend)

    def part(k, c):
        return jnp.dot(xl[k], wall[c], preferred_element_type=jnp.float32)

    def give(k, c):
        t = k * (chunks // 2) + c // 2

        @pl.when(c % 2 != y)
        def _():
            ysend[t] = part(k, c)
            copy_y(t).start()

    def take(k, c):
        t = k * (chunks // 2) + c // 2

        @pl.when((c % 2 == y) & (c // 2 != high))
        def _():
            zsend[k] = part(k, c)
            copy_y(t).wait_recv()
            zsend[k] = zsend[k] + yrecv[t]
            copy_z(k).start()

        @pl.when((c % 2 == y) & (c // 2 == high))
        def _():
            kept[k] = part(k, c)
            copy_y(t).wait_recv()
            kept[k] = kept[k] + yrecv[t]

    at = pl.ds(pl.multiple_of((odd * chunks + 2 * high + y) * span, span), span)
    bias = b[:, at]
    out_row = w2[:, at]

    def finish(k):
        copy_z(k).wait_recv()
        act = jnp.maximum(kept[k] + zrecv[k] + bias, 0.0) * out_row
        total = jnp.sum(act, axis=1, keepdims=True)
        fsend[...] = fsend[...] + jnp.where(spots == trace_of(k), total, 0.0)

    pl.semaphore_wait(far, 1)
    arrived = set()
    for kind, k, c in schedule(blocks, chunks):
        if kind == 0:
            for p in range(PARTS):
                collect(k * PARTS + p)
        elif kind == 1:
            ready(k)
        elif kind == 4:
            finish(k)
        else:
            if c not in arrived:
                arrived.add(c)
                fetch_w(c, True).wait()
                copy_w(c).wait_recv()
            (give if kind == 2 else take)(k, c)

    me = s * n_head + h
    n_dev = n_seq * n_head

    def copy_f(d):
        to = lax.rem(me + d, n_dev)
        return remote(
            frecv.at[me], frecv.at[me], s_f.at[d], r_f.at[me], to // n_head, lax.rem(to, n_head)
        )

    frecv[me] = jnp.transpose(fsend[...])[: frecv.shape[1], :]
    for d in range(1, n_dev):
        copy_f(d).start()
    for i in range(n_dev):

        @pl.when(me != i)
        def _():
            remote(frecv.at[i], frecv.at[i], s_f.at[0], r_f.at[i], across, h).wait_recv()

    sums = [frecv[i] for i in range(4)]
    for i in range(4, n_dev):
        sums[i % 4] = sums[i % 4] + frecv[i]
    logit = (sums[0] + sums[1]) + (sums[2] + sums[3])

    live = valid[...] == 1
    low = jnp.min(jnp.where(live, logit, 1e30), axis=1, keepdims=True)
    ids = lax.broadcasted_iota(jnp.int32, (traces, pairs.shape[1]), 0)
    square = (pairs.shape[1], pairs.shape[1])
    eye = lax.broadcasted_iota(jnp.int32, square, 0) == lax.broadcasted_iota(jnp.int32, square, 1)
    winner = jnp.sum(jnp.where(pairs[0:1, :] == ids, low, 0.0), axis=0, keepdims=True)
    loser = jnp.sum(jnp.where(pairs[1:2, :] == ids, low, 0.0), axis=0, keepdims=True)
    gap = jnp.sum(jnp.where(eye, winner - loser, 0.0), axis=1, keepdims=True)
    result[:traces, :steps] = jnp.where(live, logit, 0.0)
    result[:traces, steps : steps + 1] = low
    result[: pairs.shape[1], steps + 1 : steps + 2] = gap

    for c in range(chunks):
        copy_w(c).wait_send()
    for n in range(pieces):
        copy_x1(n).wait_send()
        copy_up(n).wait_send()
        copy_x3(par, n, 0).wait_send()

        @pl.when(member)
        def _():
            copy_x3(par, n, 1).wait_send()

    for t in range(blocks * chunks // 2):
        copy_y(t).wait_send()
    for k in range(blocks):
        copy_z(k).wait_send()
    for d in range(1, n_dev):
        copy_f(d).wait_send()


def fused(n_seq, n_head, hidden_states, boundary, valid, pairs, w_first, b_first, w_second):
    traces, toks, feats = hidden_states.shape
    steps = boundary.shape[1]
    depth, width = w_first.shape
    block, cols = steps // 2, width // 2
    chunks = cols // SPAN
    mine = traces * chunks // 2
    pieces = traces * PARTS
    n_dev = n_seq * n_head
    bf16, f32 = jnp.bfloat16, jnp.float32
    dma = pltpu.SemaphoreType.DMA
    vmem = pl.BlockSpec(memory_space=pltpu.VMEM)
    hbm = pl.BlockSpec(memory_space=pl.ANY)
    result = pl.pallas_call(
        functools.partial(kernel, n_seq, n_head),
        out_shape=jax.ShapeDtypeStruct((max(traces, pairs.shape[0]), steps + 64), f32),
        in_specs=[hbm] + [vmem] * 3 + [hbm] + [vmem] * 2,
        out_specs=vmem,
        scratch_shapes=[
            pltpu.VMEM((traces, toks, feats), bf16),
            pltpu.VMEM((2, traces, block, feats), bf16),
            pltpu.VMEM((traces, block, feats), bf16),
            pltpu.VMEM((traces, block, feats), bf16),
            pltpu.VMEM((traces, block, feats), bf16),
            pltpu.VMEM((2, traces, block, feats), bf16),
            pltpu.VMEM((traces, steps, feats), bf16),
            pltpu.VMEM((chunks, depth, SPAN), bf16),
            pltpu.VMEM((chunks, 2 * depth, SPAN), bf16),
            pltpu.VMEM((mine, steps, SPAN), f32),
            pltpu.VMEM((mine, steps, SPAN), f32),
            pltpu.VMEM((traces, steps, SPAN), f32),
            pltpu.VMEM((traces, steps, SPAN), f32),
            pltpu.VMEM((traces, steps, SPAN), f32),
            pltpu.VMEM((steps, 128), f32),
            pltpu.VMEM((n_dev, traces, steps), f32),
            pltpu.SemaphoreType.REGULAR,
            dma((traces,)), dma((chunks, 2)),
            dma((pieces,)), dma((pieces,)),
            dma((chunks,)), dma((chunks,)),
            dma((pieces,)), dma((pieces,)), dma((pieces,)),
            dma((2 * pieces,)), dma((2 * pieces,)),
            dma((mine,)), dma((mine,)),
            dma((traces,)), dma((traces,)),
            dma((n_dev,)), dma((n_dev,)),
        ],
        compiler_params=pltpu.CompilerParams(collective_id=0, has_side_effects=True),
    )(
        hidden_states, boundary, valid, pairs.T, w_first,
        b_first.reshape(1, width), w_second.reshape(1, width),
    )
    return result[:traces, :steps], result[:traces, steps], result[: pairs.shape[0], steps + 1]


def solution(mesh):
    n_seq, n_head = mesh.shape["seq"], mesh.shape["head"]
    paired = n_seq == 8 and n_head == 4
    body = functools.partial(fused, n_seq, n_head) if paired else per_device
    placed = (P(None, "seq", "head"), P(), P(), P(), P("seq", "head"), P("head"), P("head"))
    return jax.shard_map(
        body, mesh=mesh, in_specs=placed, out_specs=(P(), P(), P()), check_vma=False
    )
```

```python
import functools

import jax
import jax.numpy as jnp
from jax import lax
from jax.experimental import pallas as pl
from jax.experimental.pallas import tpu as pltpu
from jax.sharding import PartitionSpec as P

MESH = pl.DeviceIdType.MESH
SPAN = 128
HUB_FIRST = 0
EARLY = 1
W_MEMBER = (-8, 7, 7, 7)
W_OUTER = (-8, 7, 7, 7)
W_MIDDLE = (-8, -6, -4, -1)
PARTS = 2
END_LAG = 8
MID_LAG = 12
END_AHEAD = 2
MID_AHEAD = 1
ROW_PACE = 1.3
COLUMN_AT = (0, 5.5, 9, 10)


def row_order(blocks, chunks):
    return [(k, c) for k in range(blocks) for c in range(chunks)]


def wave_order(blocks, chunks):
    when = lambda k, c: (max(ROW_PACE * k, COLUMN_AT[c]), c, k)
    return sorted(row_order(blocks, chunks), key=lambda tile: when(*tile))


def schedule(order, blocks, lag, ahead):
    ops, got, held = [], 0, 0
    for i in range(len(order) + lag):
        if i < len(order):
            k, c = order[i]
            while got < min(blocks, k + 1 + ahead):
                ops.append((0, got, 0))
                got += 1
            while held < k + 1:
                ops.append((1, held, 0))
                held += 1
            ops.append((2, k, c))
        if i >= lag:
            ops.append((3, *order[i - lag]))
    return ops


def score_rows(rows, w_first, b_first, w_second):
    pre = jnp.dot(
        rows, lax.all_gather(w_first, "seq", axis=0, tiled=True), preferred_element_type=jnp.float32
    )
    return jnp.sum(jnp.maximum(pre + b_first, 0.0) * w_second, axis=-1)


def per_device(hidden_states, boundary, valid, pairs, w_first, b_first, w_second):
    traces, tok_dev, quarter = hidden_states.shape
    offset = lax.axis_index("seq") * tok_dev
    positions = offset + jnp.arange(tok_dev, dtype=jnp.int32)
    hits = boundary[:, :, None] == positions[None, None, :]
    whole = lax.all_gather(hidden_states, "head", axis=2, tiled=True)
    token_logit = score_rows(
        whole.reshape(traces * tok_dev, whole.shape[2]), w_first, b_first, w_second
    )
    token_logit = token_logit.reshape(traces, tok_dev)
    partial_logit = jnp.sum(jnp.where(hits, token_logit[:, None, :], 0.0), axis=2)
    logit = lax.psum(partial_logit, ("seq", "head"))
    live = valid == 1
    step_reward = jnp.where(live, logit, jnp.float32(0.0))
    trace_score = jnp.min(jnp.where(live, logit, jnp.float32(1e30)), axis=1)
    trace_ids = jnp.arange(traces, dtype=jnp.int32)[None, :]
    winner = jnp.sum(jnp.where(pairs[:, 0:1] == trace_ids, trace_score[None, :], 0.0), axis=1)
    loser = jnp.sum(jnp.where(pairs[:, 1:2] == trace_ids, trace_score[None, :], 0.0), axis=1)
    return (step_reward, trace_score, winner - loser)


def kernel(
    n_seq, n_head, hid_hbm, bnd, valid, pairs, w_hbm, b, w2, result,
    hid, xo, xin, xup, xdn, xq, xl, wown, wall,
    ysend, yrecv, zsend, zrecv, kept, whole, fsend, frecv, far,
    s_hid, s_win, s_x1, r_x1, s_w, r_w, s_x2, r_up, r_dn, s_x3, r_x3,
    s_y, r_y, s_z, r_z, s_f, r_f,
):
    traces, toks, feats = hid.shape
    blocks, block, _ = xin.shape
    steps = bnd.shape[1]
    planes = n_seq // 2
    depth = w_hbm.shape[0]
    cols = w_hbm.shape[1] // 2
    chunks, _, span = wown.shape
    groups = traces // 2
    s = lax.axis_index("seq")
    h = lax.axis_index("head")
    z = s // 2
    y = s % 2
    other = 1 - y
    odd = z % 2
    high = z // 2
    par = h % 2
    lanes = lax.broadcasted_iota(jnp.int32, (block, feats), 1)

    def fetch_w(c, mine):
        first = pl.multiple_of((odd if mine else 1 - odd) * cols + c * span, span)
        rows = pl.ds(pl.multiple_of(odd * depth, depth), depth)
        return pltpu.make_async_copy(
            w_hbm.at[:, pl.ds(first, span)],
            wall.at[c, rows, :] if mine else wown.at[c],
            s_win.at[c, 1 if mine else 0],
        )

    def trace_of(k):
        return (k % 2) * groups + k // 2

    def fetch_hid(k):
        t = trace_of(k)
        return pltpu.make_async_copy(hid_hbm.at[t], hid.at[t], s_hid.at[t])

    for k in range(blocks):
        fetch_hid(k).start()
        if k % 2 == 1 and k // 2 < chunks:
            fetch_w(k // 2, False).start()

    def remote(src, dst, send, recv, to_s, to_h):
        return pltpu.make_async_remote_copy(
            src_ref=src, dst_ref=dst, send_sem=send, recv_sem=recv,
            device_id=(to_s, to_h), device_id_type=MESH,
        )

    across = s + 1 - 2 * y
    h_core = h + 1 - 2 * par
    h_x = lax.rem(h + 2, n_head)
    s_near = s + 2 - 4 * odd
    s_far = lax.rem(s + n_seq // 2, n_seq)
    is_end = (z == 0) | (z == planes - 1)
    middle = jnp.logical_not(is_end)
    member = (h // 2) == high
    hub = member & middle

    barrier = pltpu.get_barrier_semaphore()

    def greet(to_s, to_h):
        pl.semaphore_signal(barrier, inc=1, device_id=(to_s, to_h), device_id_type=MESH)

    greet(across, h)
    greet(s, h_core)
    greet(s, h_x)

    @pl.when(z > 0)
    def _():
        greet(s - 2, h)

    @pl.when(z < planes - 1)
    def _():
        greet(s + 2, h)

    def turn(rows):
        return jnp.concatenate([rows[:, feats // 2 :], rows[:, : feats // 2]], axis=1)

    def fold(low, high_rows):
        return (
            jnp.where(lanes < feats // 2, low, turn(high_rows)),
            jnp.where(lanes < feats // 2, turn(low), high_rows),
        )

    def pick(k):
        t = trace_of(k)
        fetch_hid(k).wait()
        pos = lax.broadcasted_iota(jnp.int32, (toks, steps), 0) + s * toks
        hot = jnp.where(bnd[pl.ds(t, 1), :] == pos, 1.0, 0.0).astype(jnp.bfloat16)
        got = lax.dot_general(
            hot, hid[t], (((0,), (0,)), ((), ())), preferred_element_type=jnp.float32
        )
        pair = fold(got[:block], got[block:])
        for half in range(2):
            xo[half, k] = pair[half].astype(jnp.bfloat16)

    size = block // PARTS
    pieces = blocks * PARTS

    def rows_of(n):
        return pl.ds((n % PARTS) * size, size)

    def copy_x1(n):
        k, rows = n // PARTS, rows_of(n)
        return remote(
            xo.at[other, k, rows], xin.at[k, rows], s_x1.at[n], r_x1.at[n], across, h
        )

    def copy_w(c):
        rows = pl.ds(pl.multiple_of(odd * depth, depth), depth)
        return remote(wown.at[c], wall.at[c, rows, :], s_w.at[c], r_w.at[c], s_near, h)

    for k in range(EARLY):
        pick(k)
    pl.semaphore_wait(
        barrier, 3 + jnp.where(z > 0, 1, 0) + jnp.where(z < planes - 1, 1, 0)
    )
    def send_w(k):
        for c in range(chunks):
            for plan, who in (
                (W_MEMBER, member & is_end),
                (W_OUTER, jnp.logical_not(member) & is_end),
                (W_MIDDLE, middle),
            ):
                if plan[c] == k:

                    @pl.when(who)
                    def _():
                        fetch_w(c, False).wait()
                        copy_w(c).start()

    for k in range(blocks):
        if k >= EARLY:
            pick(k)
        for p in range(PARTS):
            copy_x1(k * PARTS + p).start()
        send_w(k - blocks)
    for c in range(chunks):
        fetch_w(c, True).start()

    @pl.when(middle)
    def _():
        pl.semaphore_signal(far, inc=1, device_id=(s - 2, h), device_id_type=MESH)
        pl.semaphore_signal(far, inc=1, device_id=(s + 2, h), device_id_type=MESH)

    def copy_up(n):
        k, rows = n // PARTS, rows_of(n)
        to_s = jnp.where(member, s_near, jnp.where(h >= n_head // 2, s + 2, s - 2))
        return remote(
            xo.at[y, k, rows], xup.at[k, rows], s_x2.at[n], r_up.at[n],
            lax.rem(to_s + n_seq, n_seq), h,
        )

    def copy_dn(n):
        k, rows = n // PARTS, rows_of(n)
        return remote(xo.at[y, k, rows], xdn.at[k, rows], s_x2.at[n], r_dn.at[n], s_near, h)

    def copy_x3(q, n, way):
        k, rows = n // PARTS, rows_of(n)
        to_h = h_x if way else h_core
        return remote(
            xq.at[q, k, rows], xq.at[q, k, rows], s_x3.at[way * pieces + n],
            r_x3.at[q * pieces + n], s, to_h,
        )

    def relay(n):
        k, rows = n // PARTS, rows_of(n)
        copy_x1(n).wait_recv()
        xo[y, k, rows] = xo[y, k, rows] + xin[k, rows]

        @pl.when(middle)
        def _():
            copy_up(n).wait_recv()
            xo[y, k, rows] = xo[y, k, rows] + xup[k, rows]

        @pl.when(member)
        def _():
            copy_dn(n).start()

        @pl.when(jnp.logical_not(member))
        def _():
            copy_up(n).start()

    def gather(n):
        k, rows = n // PARTS, rows_of(n)
        copy_x1(n).wait_recv()
        copy_up(n).wait_recv()
        xo[y, k, rows] = (xo[y, k, rows] + xin[k, rows]) + xup[k, rows]
        copy_up(n).start()
        copy_dn(n).wait_recv()
        xq[par, k, rows] = xo[y, k, rows] + xdn[k, rows]
        copy_x3(par, n, 1).start()
        copy_x3(par, n, 0).start()

    def collect(n, ends):
        k, rows = n // PARTS, rows_of(n)

        @pl.when(member)
        def _():
            if ends:
                copy_up(n).wait_recv()
                xq[par, k, rows] = xo[y, k, rows] + xup[k, rows]
                copy_x3(par, n, 1).start()
                copy_x3(par, n, 0).start()
            elif k >= HUB_FIRST:
                gather(n)

        @pl.when(jnp.logical_not(member))
        def _():
            copy_x3(par, n, 1).wait_recv()
            copy_x3(par, n, 0).start()

    def ready(k):
        for p in range(PARTS):
            copy_x3(1 - par, k * PARTS + p, 0).wait_recv()
        low = xq[0, k].astype(jnp.float32)
        top = xq[1, k].astype(jnp.float32)
        pair = fold(low, top)
        xl[k, :block] = pair[0].astype(jnp.bfloat16)
        xl[k, block:] = pair[1].astype(jnp.bfloat16)

    @pl.when(jnp.logical_not(hub))
    def _():
        for k in range(blocks):
            for p in range(PARTS):
                relay(k * PARTS + p)
            send_w(k)

    @pl.when(hub)
    def _():
        for n in range(HUB_FIRST * PARTS):
            gather(n)

    def copy_y(t):
        return remote(ysend.at[t], yrecv.at[t], s_y.at[t], r_y.at[t], across, h)

    def copy_z(t):
        return remote(zsend.at[t], zrecv.at[t], s_z.at[t], r_z.at[t], s_far, h)

    spots = lax.broadcasted_iota(jnp.int32, (steps, 128), 1)
    fsend[...] = jnp.zeros_like(fsend)

    def part(k, c):
        return jnp.dot(xl[k], wall[c], preferred_element_type=jnp.float32)

    def give(k, c):
        t = k * (chunks // 2) + c // 2

        @pl.when(y != (c + k) % 2)
        def _():
            ysend[t] = part(k, c)
            copy_y(t).start()

    def take(k, c):
        t = k * (chunks // 2) + c // 2

        @pl.when(y == (c + k) % 2)
        def _():
            kept[t] = part(k, c)
            copy_y(t).wait_recv()

            @pl.when(high != (c // 2 + k // 2) % 2)
            def _():
                zsend[k] = kept[t] + yrecv[t]
                copy_z(k).start()

            @pl.when(high == (c // 2 + k // 2) % 2)
            def _():
                whole[k] = kept[t] + yrecv[t]

    def finish(k):
        c = 2 * lax.rem(high + k // 2, 2) + lax.rem(y + k, 2)
        at = pl.ds(pl.multiple_of((odd * chunks + c) * span, span), span)
        copy_z(k).wait_recv()
        act = jnp.maximum(whole[k] + zrecv[k] + b[:, at], 0.0) * w2[:, at]
        total = jnp.sum(act, axis=1, keepdims=True)
        fsend[...] = fsend[...] + jnp.where(spots == trace_of(k), total, 0.0)

    pl.semaphore_wait(far, 1)
    def run(order, lag, ahead, ends):
        arrived = set()
        for kind, k, c in schedule(order, blocks, lag, ahead):
            if kind == 0:
                for p in range(PARTS):
                    collect(k * PARTS + p, ends)
            elif kind == 1:
                ready(k)
            else:
                if c not in arrived:
                    arrived.add(c)
                    fetch_w(c, True).wait()
                    copy_w(c).wait_recv()
                (give if kind == 2 else take)(k, c)

    @pl.when(is_end)
    def _():
        run(row_order(blocks, chunks), END_LAG, END_AHEAD, True)

    @pl.when(middle)
    def _():
        run(wave_order(blocks, chunks), MID_LAG, MID_AHEAD, False)

    for k in range(blocks):
        finish(k)

    me = s * n_head + h
    n_dev = n_seq * n_head

    def copy_f(d):
        to = lax.rem(me + d, n_dev)
        return remote(
            frecv.at[me], frecv.at[me], s_f.at[d], r_f.at[me], to // n_head, lax.rem(to, n_head)
        )

    frecv[me] = jnp.transpose(fsend[...])[: frecv.shape[1], :]
    for d in range(1, n_dev):
        copy_f(d).start()
    for c in range(chunks):
        copy_w(c).wait_send()
    for n in range(pieces):
        copy_x1(n).wait_send()
        copy_up(n).wait_send()
        copy_x3(par, n, 0).wait_send()

        @pl.when(member)
        def _():
            copy_x3(par, n, 1).wait_send()

    for t in range(blocks * chunks // 2):
        copy_y(t).wait_send()
    for k in range(blocks):
        copy_z(k).wait_send()
    for i in range(n_dev):

        @pl.when(me != i)
        def _():
            remote(frecv.at[i], frecv.at[i], s_f.at[0], r_f.at[i], across, h).wait_recv()

    sums = [frecv[i] for i in range(4)]
    for i in range(4, n_dev):
        sums[i % 4] = sums[i % 4] + frecv[i]
    logit = (sums[0] + sums[1]) + (sums[2] + sums[3])

    live = valid[...] == 1
    low = jnp.min(jnp.where(live, logit, 1e30), axis=1, keepdims=True)
    ids = lax.broadcasted_iota(jnp.int32, (traces, pairs.shape[1]), 0)
    square = (pairs.shape[1], pairs.shape[1])
    eye = lax.broadcasted_iota(jnp.int32, square, 0) == lax.broadcasted_iota(jnp.int32, square, 1)
    winner = jnp.sum(jnp.where(pairs[0:1, :] == ids, low, 0.0), axis=0, keepdims=True)
    loser = jnp.sum(jnp.where(pairs[1:2, :] == ids, low, 0.0), axis=0, keepdims=True)
    gap = jnp.sum(jnp.where(eye, winner - loser, 0.0), axis=1, keepdims=True)
    result[:traces, :steps] = jnp.where(live, logit, 0.0)
    result[:traces, steps : steps + 1] = low
    result[: pairs.shape[1], steps + 1 : steps + 2] = gap

    for d in range(1, n_dev):
        copy_f(d).wait_send()


def fused(n_seq, n_head, hidden_states, boundary, valid, pairs, w_first, b_first, w_second):
    traces, toks, feats = hidden_states.shape
    steps = boundary.shape[1]
    depth, width = w_first.shape
    block, cols = steps // 2, width // 2
    chunks = cols // SPAN
    mine = traces * chunks // 2
    pieces = traces * PARTS
    n_dev = n_seq * n_head
    bf16, f32 = jnp.bfloat16, jnp.float32
    dma = pltpu.SemaphoreType.DMA
    vmem = pl.BlockSpec(memory_space=pltpu.VMEM)
    hbm = pl.BlockSpec(memory_space=pl.ANY)
    result = pl.pallas_call(
        functools.partial(kernel, n_seq, n_head),
        out_shape=jax.ShapeDtypeStruct((max(traces, pairs.shape[0]), steps + 64), f32),
        in_specs=[hbm] + [vmem] * 3 + [hbm] + [vmem] * 2,
        out_specs=vmem,
        scratch_shapes=[
            pltpu.VMEM((traces, toks, feats), bf16),
            pltpu.VMEM((2, traces, block, feats), bf16),
            pltpu.VMEM((traces, block, feats), bf16),
            pltpu.VMEM((traces, block, feats), bf16),
            pltpu.VMEM((traces, block, feats), bf16),
            pltpu.VMEM((2, traces, block, feats), bf16),
            pltpu.VMEM((traces, steps, feats), bf16),
            pltpu.VMEM((chunks, depth, SPAN), bf16),
            pltpu.VMEM((chunks, 2 * depth, SPAN), bf16),
            pltpu.VMEM((mine, steps, SPAN), f32),
            pltpu.VMEM((mine, steps, SPAN), f32),
            pltpu.VMEM((traces, steps, SPAN), f32),
            pltpu.VMEM((traces, steps, SPAN), f32),
            pltpu.VMEM((mine, steps, SPAN), f32),
            pltpu.VMEM((traces, steps, SPAN), f32),
            pltpu.VMEM((steps, 128), f32),
            pltpu.VMEM((n_dev, traces, steps), f32),
            pltpu.SemaphoreType.REGULAR,
            dma((traces,)), dma((chunks, 2)),
            dma((pieces,)), dma((pieces,)),
            dma((chunks,)), dma((chunks,)),
            dma((pieces,)), dma((pieces,)), dma((pieces,)),
            dma((2 * pieces,)), dma((2 * pieces,)),
            dma((mine,)), dma((mine,)),
            dma((traces,)), dma((traces,)),
            dma((n_dev,)), dma((n_dev,)),
        ],
        compiler_params=pltpu.CompilerParams(collective_id=0, has_side_effects=True),
    )(
        hidden_states, boundary, valid, pairs.T, w_first,
        b_first.reshape(1, width), w_second.reshape(1, width),
    )
    return result[:traces, :steps], result[:traces, steps], result[: pairs.shape[0], steps + 1]


def solution(mesh):
    n_seq, n_head = mesh.shape["seq"], mesh.shape["head"]
    paired = n_seq == 8 and n_head == 4
    body = functools.partial(fused, n_seq, n_head) if paired else per_device
    placed = (P(None, "seq", "head"), P(), P(), P(), P("seq", "head"), P("head"), P("head"))
    return jax.shard_map(
        body, mesh=mesh, in_specs=placed, out_specs=(P(), P(), P()), check_vma=False
    )
```

```python
import functools

import jax
import jax.numpy as jnp
from jax import lax
from jax.experimental import pallas as pl
from jax.experimental.pallas import tpu as pltpu
from jax.sharding import PartitionSpec as P

MESH = pl.DeviceIdType.MESH
SPAN = 128
HUB_FIRST = 0
EARLY = 1
W_MEMBER = (-8, 7, 7, 7)
W_OUTER = (-8, 7, 7, 7)
W_MIDDLE = (-8, -6, -4, -1)
PARTS = 2
LEAN_A = (6, 7)
LEAN_B = (7,)
END_LAG = 8
MID_LAG = 12
END_AHEAD = 2
MID_AHEAD = 1
ROW_PACE = 1.3
COLUMN_AT = (0, 5.5, 9, 10)


def row_order(blocks, chunks):
    return [(k, c) for k in range(blocks) for c in range(chunks)]


def wave_order(blocks, chunks):
    when = lambda k, c: (max(ROW_PACE * k, COLUMN_AT[c]), c, k)
    return sorted(row_order(blocks, chunks), key=lambda tile: when(*tile))


def schedule(order, blocks, lag, ahead):
    ops, got, held = [], 0, 0
    for i in range(len(order) + lag):
        if i < len(order):
            k, c = order[i]
            while got < min(blocks, k + 1 + ahead):
                ops.append((0, got, 0))
                got += 1
            while held < k + 1:
                ops.append((1, held, 0))
                held += 1
            ops.append((2, k, c))
        if i >= lag:
            ops.append((3, *order[i - lag]))
    return ops


def score_rows(rows, w_first, b_first, w_second):
    pre = jnp.dot(
        rows, lax.all_gather(w_first, "seq", axis=0, tiled=True), preferred_element_type=jnp.float32
    )
    return jnp.sum(jnp.maximum(pre + b_first, 0.0) * w_second, axis=-1)


def per_device(hidden_states, boundary, valid, pairs, w_first, b_first, w_second):
    traces, tok_dev, quarter = hidden_states.shape
    offset = lax.axis_index("seq") * tok_dev
    positions = offset + jnp.arange(tok_dev, dtype=jnp.int32)
    hits = boundary[:, :, None] == positions[None, None, :]
    whole = lax.all_gather(hidden_states, "head", axis=2, tiled=True)
    token_logit = score_rows(
        whole.reshape(traces * tok_dev, whole.shape[2]), w_first, b_first, w_second
    )
    token_logit = token_logit.reshape(traces, tok_dev)
    partial_logit = jnp.sum(jnp.where(hits, token_logit[:, None, :], 0.0), axis=2)
    logit = lax.psum(partial_logit, ("seq", "head"))
    live = valid == 1
    step_reward = jnp.where(live, logit, jnp.float32(0.0))
    trace_score = jnp.min(jnp.where(live, logit, jnp.float32(1e30)), axis=1)
    trace_ids = jnp.arange(traces, dtype=jnp.int32)[None, :]
    winner = jnp.sum(jnp.where(pairs[:, 0:1] == trace_ids, trace_score[None, :], 0.0), axis=1)
    loser = jnp.sum(jnp.where(pairs[:, 1:2] == trace_ids, trace_score[None, :], 0.0), axis=1)
    return (step_reward, trace_score, winner - loser)


def kernel(
    n_seq, n_head, hid_hbm, bnd, valid, pairs, w_hbm, b, w2, result,
    hid, xo, xin, xup, xdn, xq, xl, wown, wall,
    ysend, yrecv, zsend, zrecv, kept, fsend, frecv, far,
    s_hid, s_win, s_x1, r_x1, s_w, r_w, s_x2, r_up, r_dn, s_x3, r_x3,
    s_y, r_y, s_z, r_z, s_f, r_f,
):
    traces, toks, feats = hid.shape
    blocks, block, _ = xin.shape
    steps = bnd.shape[1]
    planes = n_seq // 2
    depth = w_hbm.shape[0]
    cols = w_hbm.shape[1] // 2
    chunks, _, span = wown.shape
    groups = traces // 2
    s = lax.axis_index("seq")
    h = lax.axis_index("head")
    z = s // 2
    y = s % 2
    other = 1 - y
    odd = z % 2
    high = z // 2
    par = h % 2
    lanes = lax.broadcasted_iota(jnp.int32, (block, feats), 1)

    def fetch_w(c, mine):
        first = pl.multiple_of((odd if mine else 1 - odd) * cols + c * span, span)
        rows = pl.ds(pl.multiple_of(odd * depth, depth), depth)
        return pltpu.make_async_copy(
            w_hbm.at[:, pl.ds(first, span)],
            wall.at[c, rows, :] if mine else wown.at[c],
            s_win.at[c, 1 if mine else 0],
        )

    def trace_of(k):
        return (k % 2) * groups + k // 2

    def fetch_hid(k):
        t = trace_of(k)
        return pltpu.make_async_copy(hid_hbm.at[t], hid.at[t], s_hid.at[t])

    for k in range(blocks):
        fetch_hid(k).start()
        if k % 2 == 1 and k // 2 < chunks:
            fetch_w(k // 2, False).start()

    def remote(src, dst, send, recv, to_s, to_h):
        return pltpu.make_async_remote_copy(
            src_ref=src, dst_ref=dst, send_sem=send, recv_sem=recv,
            device_id=(to_s, to_h), device_id_type=MESH,
        )

    across = s + 1 - 2 * y
    h_core = h + 1 - 2 * par
    h_x = lax.rem(h + 2, n_head)
    s_near = s + 2 - 4 * odd
    s_far = lax.rem(s + n_seq // 2, n_seq)
    is_end = (z == 0) | (z == planes - 1)
    middle = jnp.logical_not(is_end)
    member = (h // 2) == high
    hub = member & middle

    barrier = pltpu.get_barrier_semaphore()

    def greet(to_s, to_h):
        pl.semaphore_signal(barrier, inc=1, device_id=(to_s, to_h), device_id_type=MESH)

    greet(across, h)
    greet(s, h_core)
    greet(s, h_x)

    @pl.when(z > 0)
    def _():
        greet(s - 2, h)

    @pl.when(z < planes - 1)
    def _():
        greet(s + 2, h)

    def turn(rows):
        return jnp.concatenate([rows[:, feats // 2 :], rows[:, : feats // 2]], axis=1)

    def fold(low, high_rows):
        return (
            jnp.where(lanes < feats // 2, low, turn(high_rows)),
            jnp.where(lanes < feats // 2, turn(low), high_rows),
        )

    def pick(k):
        t = trace_of(k)
        fetch_hid(k).wait()
        pos = lax.broadcasted_iota(jnp.int32, (toks, steps), 0) + s * toks
        hot = jnp.where(bnd[pl.ds(t, 1), :] == pos, 1.0, 0.0).astype(jnp.bfloat16)
        got = lax.dot_general(
            hot, hid[t], (((0,), (0,)), ((), ())), preferred_element_type=jnp.float32
        )
        pair = fold(got[:block], got[block:])
        for half in range(2):
            xo[half, k] = pair[half].astype(jnp.bfloat16)

    size = block // PARTS
    pieces = blocks * PARTS

    def rows_of(n):
        return pl.ds((n % PARTS) * size, size)

    def copy_x1(n):
        k, rows = n // PARTS, rows_of(n)
        return remote(
            xo.at[other, k, rows], xin.at[k, rows], s_x1, r_x1.at[n], across, h
        )

    def copy_w(c):
        rows = pl.ds(pl.multiple_of(odd * depth, depth), depth)
        return remote(wown.at[c], wall.at[c, rows, :], s_w, r_w.at[c], s_near, h)

    for k in range(EARLY):
        pick(k)
    pl.semaphore_wait(
        barrier, 3 + jnp.where(z > 0, 1, 0) + jnp.where(z < planes - 1, 1, 0)
    )
    def send_w(k):
        for c in range(chunks):
            for plan, who in (
                (W_MEMBER, member & is_end),
                (W_OUTER, jnp.logical_not(member) & is_end),
                (W_MIDDLE, middle),
            ):
                if plan[c] == k:

                    @pl.when(who)
                    def _():
                        fetch_w(c, False).wait()
                        copy_w(c).start()

    for k in range(blocks):
        if k >= EARLY:
            pick(k)
        for p in range(PARTS):
            copy_x1(k * PARTS + p).start()
        send_w(k - blocks)
    for c in range(chunks):
        fetch_w(c, True).start()

    @pl.when(middle)
    def _():
        pl.semaphore_signal(far, inc=1, device_id=(s - 2, h), device_id_type=MESH)
        pl.semaphore_signal(far, inc=1, device_id=(s + 2, h), device_id_type=MESH)

    def copy_up(n):
        k, rows = n // PARTS, rows_of(n)
        to_s = jnp.where(member, s_near, jnp.where(h >= n_head // 2, s + 2, s - 2))
        return remote(
            xo.at[y, k, rows], xup.at[k, rows], s_x2, r_up.at[n],
            lax.rem(to_s + n_seq, n_seq), h,
        )

    def copy_dn(n):
        k, rows = n // PARTS, rows_of(n)
        return remote(xo.at[y, k, rows], xdn.at[k, rows], s_x2, r_dn.at[n], s_near, h)

    def copy_x3(q, n, way):
        k, rows = n // PARTS, rows_of(n)
        to_h = h_x if way else h_core
        return remote(
            xq.at[q, k, rows], xq.at[q, k, rows], s_x3.at[way],
            r_x3.at[q * pieces + n], s, to_h,
        )

    def relay(n):
        k, rows = n // PARTS, rows_of(n)
        copy_x1(n).wait_recv()
        xo[y, k, rows] = xo[y, k, rows] + xin[k, rows]

        @pl.when(middle)
        def _():
            copy_up(n).wait_recv()
            xo[y, k, rows] = xo[y, k, rows] + xup[k, rows]

        @pl.when(member)
        def _():
            copy_dn(n).start()

        @pl.when(jnp.logical_not(member))
        def _():
            copy_up(n).start()

    def gather(n):
        k, rows = n // PARTS, rows_of(n)
        copy_x1(n).wait_recv()
        copy_up(n).wait_recv()
        xo[y, k, rows] = (xo[y, k, rows] + xin[k, rows]) + xup[k, rows]
        copy_up(n).start()
        copy_dn(n).wait_recv()
        xq[par, k, rows] = xo[y, k, rows] + xdn[k, rows]
        copy_x3(par, n, 1).start()
        copy_x3(par, n, 0).start()

    def collect(n, ends):
        k, rows = n // PARTS, rows_of(n)

        @pl.when(member)
        def _():
            if ends:
                copy_up(n).wait_recv()
                xq[par, k, rows] = xo[y, k, rows] + xup[k, rows]
                copy_x3(par, n, 1).start()
                copy_x3(par, n, 0).start()
            elif k >= HUB_FIRST:
                gather(n)

        @pl.when(jnp.logical_not(member))
        def _():
            copy_x3(par, n, 1).wait_recv()
            copy_x3(par, n, 0).start()

    def ready(k):
        for p in range(PARTS):
            copy_x3(1 - par, k * PARTS + p, 0).wait_recv()
        low = xq[0, k].astype(jnp.float32)
        top = xq[1, k].astype(jnp.float32)
        pair = fold(low, top)
        xl[k, :block] = pair[0].astype(jnp.bfloat16)
        xl[k, block:] = pair[1].astype(jnp.bfloat16)

    @pl.when(jnp.logical_not(hub))
    def _():
        for k in range(blocks):
            for p in range(PARTS):
                relay(k * PARTS + p)
            send_w(k)

    @pl.when(hub)
    def _():
        for n in range(HUB_FIRST * PARTS):
            gather(n)

    def copy_y(t):
        return remote(ysend.at[t], yrecv.at[t], s_y, r_y.at[t], across, h)

    def copy_z(t):
        return remote(zsend.at[t], zrecv.at[t], s_z, r_z.at[t], s_far, h)

    spots = lax.broadcasted_iota(jnp.int32, (steps, 128), 1)
    fsend[...] = jnp.zeros_like(fsend)

    def part(k, c):
        return jnp.dot(xl[k], wall[c], preferred_element_type=jnp.float32)

    def owner_of(k, j):
        base = (j + k // 2) % 2
        return (1 if k in LEAN_A else base, 0 if k in LEAN_B else base)

    def owner(k, j):
        return jnp.where(h < n_head // 2, *owner_of(k, j))

    def give(k, c):
        t = k * (chunks // 2) + c // 2

        @pl.when(y != (c + k) % 2)
        def _():
            ysend[t] = part(k, c)
            copy_y(t).start()

    def take(k, c):
        t = k * (chunks // 2) + c // 2

        @pl.when(y == (c + k) % 2)
        def _():
            kept[t] = part(k, c)
            copy_y(t).wait_recv()

            @pl.when(high != owner(k, c // 2))
            def _():
                zsend[t] = kept[t] + yrecv[t]
                copy_z(t).start()

            @pl.when(high == owner(k, c // 2))
            def _():
                kept[t] = kept[t] + yrecv[t]

    def finish(k, j):
        c = 2 * j + lax.rem(y + k, 2)
        t = k * (chunks // 2) + j

        @pl.when(high == owner(k, j))
        def _():
            at = pl.ds(pl.multiple_of((odd * chunks + c) * span, span), span)
            copy_z(t).wait_recv()
            act = jnp.maximum(kept[t] + zrecv[t] + b[:, at], 0.0) * w2[:, at]
            total = jnp.sum(act, axis=1, keepdims=True)
            fsend[...] = fsend[...] + jnp.where(spots == trace_of(k), total, 0.0)

    pl.semaphore_wait(far, 1)
    def run(order, lag, ahead, ends):
        arrived = set()
        for kind, k, c in schedule(order, blocks, lag, ahead):
            if kind == 0:
                for p in range(PARTS):
                    collect(k * PARTS + p, ends)
            elif kind == 1:
                ready(k)
            else:
                if c not in arrived:
                    arrived.add(c)
                    fetch_w(c, True).wait()
                    copy_w(c).wait_recv()
                (give if kind == 2 else take)(k, c)

    @pl.when(is_end)
    def _():
        run(row_order(blocks, chunks), END_LAG, END_AHEAD, True)

    @pl.when(middle)
    def _():
        run(wave_order(blocks, chunks), MID_LAG, MID_AHEAD, False)

    for k in range(blocks):
        for j in range(chunks // 2):
            finish(k, j)

    me = s * n_head + h
    n_dev = n_seq * n_head

    def copy_f(d):
        to = lax.rem(me + d, n_dev)
        return remote(
            frecv.at[me], frecv.at[me], s_f, r_f, to // n_head, lax.rem(to, n_head)
        )

    frecv[me] = jnp.transpose(fsend[...])[: frecv.shape[1], :]
    for d in range(1, n_dev):
        copy_f(d).start()
    def drain(ref, sem):
        remote(ref, ref, sem, r_f, across, h).wait_send()

    drain(wown, s_w)
    drain(xin, s_x1)
    drain(xin, s_x2)
    drain(xin, s_x3.at[0])

    @pl.when(member)
    def _():
        drain(xin, s_x3.at[1])

    drain(ysend, s_y)
    left = h < n_head // 2
    for side in range(2):
        for up in range(2):
            sent = sum(
                up != owner_of(k, j)[side] for k in range(blocks) for j in range(chunks // 2)
            )

            @pl.when((left == (side == 0)) & (high == up))
            def _():
                drain(zsend.at[pl.ds(0, sent)], s_z)

    others = frecv.at[pl.ds(0, n_dev - 1)]
    remote(others, others, s_f, r_f, across, h).wait_recv()

    sums = [frecv[i] for i in range(4)]
    for i in range(4, n_dev):
        sums[i % 4] = sums[i % 4] + frecv[i]
    logit = (sums[0] + sums[1]) + (sums[2] + sums[3])

    live = valid[...] == 1
    low = jnp.min(jnp.where(live, logit, 1e30), axis=1, keepdims=True)
    ids = lax.broadcasted_iota(jnp.int32, (traces, pairs.shape[1]), 0)
    square = (pairs.shape[1], pairs.shape[1])
    eye = lax.broadcasted_iota(jnp.int32, square, 0) == lax.broadcasted_iota(jnp.int32, square, 1)
    winner = jnp.sum(jnp.where(pairs[0:1, :] == ids, low, 0.0), axis=0, keepdims=True)
    loser = jnp.sum(jnp.where(pairs[1:2, :] == ids, low, 0.0), axis=0, keepdims=True)
    gap = jnp.sum(jnp.where(eye, winner - loser, 0.0), axis=1, keepdims=True)
    result[:traces, :steps] = jnp.where(live, logit, 0.0)
    result[:traces, steps : steps + 1] = low
    result[: pairs.shape[1], steps + 1 : steps + 2] = gap

    drain(others, s_f)


def fused(n_seq, n_head, hidden_states, boundary, valid, pairs, w_first, b_first, w_second):
    traces, toks, feats = hidden_states.shape
    steps = boundary.shape[1]
    depth, width = w_first.shape
    block, cols = steps // 2, width // 2
    chunks = cols // SPAN
    mine = traces * chunks // 2
    pieces = traces * PARTS
    n_dev = n_seq * n_head
    bf16, f32 = jnp.bfloat16, jnp.float32
    dma = pltpu.SemaphoreType.DMA
    vmem = pl.BlockSpec(memory_space=pltpu.VMEM)
    hbm = pl.BlockSpec(memory_space=pl.ANY)
    result = pl.pallas_call(
        functools.partial(kernel, n_seq, n_head),
        out_shape=jax.ShapeDtypeStruct((max(traces, pairs.shape[0]), steps + 64), f32),
        in_specs=[hbm] + [vmem] * 3 + [hbm] + [vmem] * 2,
        out_specs=vmem,
        scratch_shapes=[
            pltpu.VMEM((traces, toks, feats), bf16),
            pltpu.VMEM((2, traces, block, feats), bf16),
            pltpu.VMEM((traces, block, feats), bf16),
            pltpu.VMEM((traces, block, feats), bf16),
            pltpu.VMEM((traces, block, feats), bf16),
            pltpu.VMEM((2, traces, block, feats), bf16),
            pltpu.VMEM((traces, steps, feats), bf16),
            pltpu.VMEM((chunks, depth, SPAN), bf16),
            pltpu.VMEM((chunks, 2 * depth, SPAN), bf16),
            pltpu.VMEM((mine, steps, SPAN), f32),
            pltpu.VMEM((mine, steps, SPAN), f32),
            pltpu.VMEM((mine, steps, SPAN), f32),
            pltpu.VMEM((mine, steps, SPAN), f32),
            pltpu.VMEM((mine, steps, SPAN), f32),
            pltpu.VMEM((steps, 128), f32),
            pltpu.VMEM((n_dev, traces, steps), f32),
            pltpu.SemaphoreType.REGULAR,
            dma((traces,)), dma((chunks, 2)),
            dma, dma((pieces,)),
            dma, dma((chunks,)),
            dma, dma((pieces,)), dma((pieces,)),
            dma((2,)), dma((2 * pieces,)),
            dma, dma((mine,)),
            dma, dma((mine,)),
            dma, dma,
        ],
        compiler_params=pltpu.CompilerParams(collective_id=0, has_side_effects=True),
    )(
        hidden_states, boundary, valid, pairs.T, w_first,
        b_first.reshape(1, width), w_second.reshape(1, width),
    )
    return result[:traces, :steps], result[:traces, steps], result[: pairs.shape[0], steps + 1]


def solution(mesh):
    n_seq, n_head = mesh.shape["seq"], mesh.shape["head"]
    paired = n_seq == 8 and n_head == 4
    body = functools.partial(fused, n_seq, n_head) if paired else per_device
    placed = (P(None, "seq", "head"), P(), P(), P(), P("seq", "head"), P("head"), P("head"))
    return jax.shard_map(
        body, mesh=mesh, in_specs=placed, out_specs=(P(), P(), P()), check_vma=False
    )
```

```python
import functools

import jax
import jax.numpy as jnp
from jax import lax
from jax.experimental import pallas as pl
from jax.experimental.pallas import tpu as pltpu
from jax.sharding import PartitionSpec as P

MESH = pl.DeviceIdType.MESH
SPAN = 128
HUB_FIRST = 4
EARLY = 1
W_MEMBER = (-8, 7, 7, 7)
W_OUTER = (-8, 7, 7, 7)
W_MIDDLE = (-8, -6, -4, -1)
PARTS = 2
LEAN_A = (6, 7)
LEAN_B = (7,)
END_LAG = 8
MID_LAG = 12
END_AHEAD = 2
MID_AHEAD = 1
ROW_PACE = 1.3
COLUMN_AT = (0, 5.5, 9, 10)


def row_order(blocks, chunks):
    return [(k, c) for k in range(blocks) for c in range(chunks)]


def wave_order(blocks, chunks):
    when = lambda k, c: (max(ROW_PACE * k, COLUMN_AT[c]), c, k)
    return sorted(row_order(blocks, chunks), key=lambda tile: when(*tile))


def schedule(order, blocks, lag, ahead):
    ops, got, held = [], 0, 0
    for i in range(len(order) + lag):
        if i < len(order):
            k, c = order[i]
            while got < min(blocks, k + 1 + ahead):
                ops.append((0, got, 0))
                got += 1
            while held < k + 1:
                ops.append((1, held, 0))
                held += 1
            ops.append((2, k, c))
        if i >= lag:
            ops.append((3, *order[i - lag]))
    return ops


def score_rows(rows, w_first, b_first, w_second):
    pre = jnp.dot(
        rows, lax.all_gather(w_first, "seq", axis=0, tiled=True), preferred_element_type=jnp.float32
    )
    return jnp.sum(jnp.maximum(pre + b_first, 0.0) * w_second, axis=-1)


def per_device(hidden_states, boundary, valid, pairs, w_first, b_first, w_second):
    traces, tok_dev, quarter = hidden_states.shape
    offset = lax.axis_index("seq") * tok_dev
    positions = offset + jnp.arange(tok_dev, dtype=jnp.int32)
    hits = boundary[:, :, None] == positions[None, None, :]
    whole = lax.all_gather(hidden_states, "head", axis=2, tiled=True)
    token_logit = score_rows(
        whole.reshape(traces * tok_dev, whole.shape[2]), w_first, b_first, w_second
    )
    token_logit = token_logit.reshape(traces, tok_dev)
    partial_logit = jnp.sum(jnp.where(hits, token_logit[:, None, :], 0.0), axis=2)
    logit = lax.psum(partial_logit, ("seq", "head"))
    live = valid == 1
    step_reward = jnp.where(live, logit, jnp.float32(0.0))
    trace_score = jnp.min(jnp.where(live, logit, jnp.float32(1e30)), axis=1)
    trace_ids = jnp.arange(traces, dtype=jnp.int32)[None, :]
    winner = jnp.sum(jnp.where(pairs[:, 0:1] == trace_ids, trace_score[None, :], 0.0), axis=1)
    loser = jnp.sum(jnp.where(pairs[:, 1:2] == trace_ids, trace_score[None, :], 0.0), axis=1)
    return (step_reward, trace_score, winner - loser)


def kernel(
    n_seq, n_head, hid_hbm, bnd, valid, pairs, w_hbm, b, w2, result,
    hid, xo, xin, xup, xdn, xq, xl, wown, wall,
    ysend, yrecv, zsend, zrecv, kept, fsend, frecv, far,
    s_hid, s_win, s_x1, r_x1, s_w, r_w, s_x2, r_up, r_dn, s_x3, r_x3,
    s_y, r_y, s_z, r_z, s_f, r_f,
):
    traces, toks, feats = hid.shape
    blocks, block, _ = xin.shape
    steps = bnd.shape[1]
    planes = n_seq // 2
    depth = w_hbm.shape[0]
    cols = w_hbm.shape[1] // 2
    chunks, _, span = wown.shape
    groups = traces // 2
    s = lax.axis_index("seq")
    h = lax.axis_index("head")
    z = s // 2
    y = s % 2
    other = 1 - y
    odd = z % 2
    high = z // 2
    par = h % 2
    lanes = lax.broadcasted_iota(jnp.int32, (block, feats), 1)

    def fetch_w(c, mine):
        first = pl.multiple_of((odd if mine else 1 - odd) * cols + c * span, span)
        rows = pl.ds(pl.multiple_of(odd * depth, depth), depth)
        return pltpu.make_async_copy(
            w_hbm.at[:, pl.ds(first, span)],
            wall.at[c, rows, :] if mine else wown.at[c],
            s_win.at[chunks if mine else c],
        )

    def trace_of(k):
        return (k % 2) * groups + k // 2

    def fetch_hid(k):
        t = trace_of(k)
        return pltpu.make_async_copy(hid_hbm.at[t], hid.at[t], s_hid.at[t])

    for k in range(blocks):
        fetch_hid(k).start()
        if k % 2 == 1 and k // 2 < chunks:
            fetch_w(k // 2, False).start()

    def remote(src, dst, send, recv, to_s, to_h):
        return pltpu.make_async_remote_copy(
            src_ref=src, dst_ref=dst, send_sem=send, recv_sem=recv,
            device_id=(to_s, to_h), device_id_type=MESH,
        )

    across = s + 1 - 2 * y
    h_core = h + 1 - 2 * par
    h_x = lax.rem(h + 2, n_head)
    s_near = s + 2 - 4 * odd
    s_far = lax.rem(s + n_seq // 2, n_seq)
    is_end = (z == 0) | (z == planes - 1)
    middle = jnp.logical_not(is_end)
    member = (h // 2) == high
    hub = member & middle

    barrier = pltpu.get_barrier_semaphore()

    def greet(to_s, to_h):
        pl.semaphore_signal(barrier, inc=1, device_id=(to_s, to_h), device_id_type=MESH)

    greet(across, h)
    greet(s, h_core)
    greet(s, h_x)

    @pl.when(z > 0)
    def _():
        greet(s - 2, h)

    @pl.when(z < planes - 1)
    def _():
        greet(s + 2, h)

    def turn(rows):
        return jnp.concatenate([rows[:, feats // 2 :], rows[:, : feats // 2]], axis=1)

    def fold(low, high_rows):
        return (
            jnp.where(lanes < feats // 2, low, turn(high_rows)),
            jnp.where(lanes < feats // 2, turn(low), high_rows),
        )

    def pick(k):
        t = trace_of(k)
        fetch_hid(k).wait()
        pos = lax.broadcasted_iota(jnp.int32, (toks, steps), 0) + s * toks
        hot = jnp.where(bnd[pl.ds(t, 1), :] == pos, 1.0, 0.0).astype(jnp.bfloat16)
        got = lax.dot_general(
            hot, hid[t], (((0,), (0,)), ((), ())), preferred_element_type=jnp.float32
        )
        pair = fold(got[:block], got[block:])
        for half in range(2):
            xo[half, k] = pair[half].astype(jnp.bfloat16)

    size = block // PARTS
    pieces = blocks * PARTS

    def rows_of(n):
        return pl.ds((n % PARTS) * size, size)

    def copy_x1(n):
        k, rows = n // PARTS, rows_of(n)
        return remote(
            xo.at[other, k, rows], xin.at[k, rows], s_x1, r_x1.at[n], across, h
        )

    def copy_w(c):
        rows = pl.ds(pl.multiple_of(odd * depth, depth), depth)
        return remote(wown.at[c], wall.at[c, rows, :], s_w, r_w.at[c], s_near, h)

    for k in range(EARLY):
        pick(k)
    pl.semaphore_wait(
        barrier, 3 + jnp.where(z > 0, 1, 0) + jnp.where(z < planes - 1, 1, 0)
    )
    def send_w(k):
        for c in range(chunks):
            for plan, who in (
                (W_MEMBER, member & is_end),
                (W_OUTER, jnp.logical_not(member) & is_end),
                (W_MIDDLE, middle),
            ):
                if plan[c] == k:

                    @pl.when(who)
                    def _():
                        fetch_w(c, False).wait()
                        copy_w(c).start()

    for k in range(blocks):
        if k >= EARLY:
            pick(k)
        for p in range(PARTS):
            copy_x1(k * PARTS + p).start()
        send_w(k - blocks)
    for c in range(chunks):
        fetch_w(c, True).start()

    @pl.when(middle)
    def _():
        pl.semaphore_signal(far, inc=1, device_id=(s - 2, h), device_id_type=MESH)
        pl.semaphore_signal(far, inc=1, device_id=(s + 2, h), device_id_type=MESH)

    def copy_up(n):
        k, rows = n // PARTS, rows_of(n)
        to_s = jnp.where(member, s_near, jnp.where(h >= n_head // 2, s + 2, s - 2))
        return remote(
            xo.at[y, k, rows], xup.at[k, rows], s_x2, r_up.at[n],
            lax.rem(to_s + n_seq, n_seq), h,
        )

    def copy_dn(n):
        k, rows = n // PARTS, rows_of(n)
        return remote(xo.at[y, k, rows], xdn.at[k, rows], s_x2, r_dn.at[n], s_near, h)

    def copy_x3(q, n, way):
        k, rows = n // PARTS, rows_of(n)
        to_h = h_x if way else h_core
        return remote(
            xq.at[q, k, rows], xq.at[q, k, rows], s_x3.at[way],
            r_x3.at[n if way else pieces + k], s, to_h,
        )

    def relay(n):
        k, rows = n // PARTS, rows_of(n)
        copy_x1(n).wait_recv()
        xo[y, k, rows] = xo[y, k, rows] + xin[k, rows]

        @pl.when(middle)
        def _():
            copy_up(n).wait_recv()
            xo[y, k, rows] = xo[y, k, rows] + xup[k, rows]

        @pl.when(member)
        def _():
            copy_dn(n).start()

        @pl.when(jnp.logical_not(member))
        def _():
            copy_up(n).start()

    def gather(n):
        k, rows = n // PARTS, rows_of(n)
        copy_x1(n).wait_recv()
        copy_up(n).wait_recv()
        xo[y, k, rows] = (xo[y, k, rows] + xin[k, rows]) + xup[k, rows]
        copy_up(n).start()
        copy_dn(n).wait_recv()
        xq[par, k, rows] = xo[y, k, rows] + xdn[k, rows]
        copy_x3(par, n, 1).start()
        copy_x3(par, n, 0).start()

    def collect(n, ends):
        k, rows = n // PARTS, rows_of(n)

        @pl.when(member)
        def _():
            if ends:
                copy_up(n).wait_recv()
                xq[par, k, rows] = xo[y, k, rows] + xup[k, rows]
                copy_x3(par, n, 1).start()
                copy_x3(par, n, 0).start()
            elif k >= HUB_FIRST:
                gather(n)

        @pl.when(jnp.logical_not(member))
        def _():
            copy_x3(par, n, 1).wait_recv()
            copy_x3(par, n, 0).start()

    def ready(k):
        both = xq.at[1 - par, k]
        remote(both, both, s_x3.at[0], r_x3.at[pieces + k], s, h_core).wait_recv()
        low = xq[0, k].astype(jnp.float32)
        top = xq[1, k].astype(jnp.float32)
        pair = fold(low, top)
        xl[k, :block] = pair[0].astype(jnp.bfloat16)
        xl[k, block:] = pair[1].astype(jnp.bfloat16)

    @pl.when(jnp.logical_not(hub))
    def _():
        for k in range(blocks):
            for p in range(PARTS):
                relay(k * PARTS + p)
            send_w(k)

    @pl.when(hub)
    def _():
        for n in range(HUB_FIRST * PARTS):
            gather(n)

    def copy_y(t):
        return remote(ysend.at[t], yrecv.at[t], s_y, r_y.at[t], across, h)

    def copy_z(t):
        return remote(zsend.at[t], zrecv.at[t], s_z, r_z.at[t], s_far, h)

    spots = lax.broadcasted_iota(jnp.int32, (steps, 128), 1)
    fsend[...] = jnp.zeros_like(fsend)

    def part(k, c):
        return jnp.dot(xl[k], wall[c], preferred_element_type=jnp.float32)

    def owner_of(k, j):
        base = (j + k // 2) % 2
        return (1 if k in LEAN_A else base, 0 if k in LEAN_B else base)

    def owner(k, j):
        return jnp.where(h < n_head // 2, *owner_of(k, j))

    def give(k, c):
        t = k * (chunks // 2) + c // 2

        @pl.when(y != (c + k) % 2)
        def _():
            ysend[t] = part(k, c)
            copy_y(t).start()

    def take(k, c):
        t = k * (chunks // 2) + c // 2

        @pl.when(y == (c + k) % 2)
        def _():
            kept[t] = part(k, c)
            copy_y(t).wait_recv()

            @pl.when(high != owner(k, c // 2))
            def _():
                zsend[t] = kept[t] + yrecv[t]
                copy_z(t).start()

            @pl.when(high == owner(k, c // 2))
            def _():
                kept[t] = kept[t] + yrecv[t]

    def finish(k, j):
        c = 2 * j + lax.rem(y + k, 2)
        t = k * (chunks // 2) + j

        @pl.when(high == owner(k, j))
        def _():
            at = pl.ds(pl.multiple_of((odd * chunks + c) * span, span), span)
            copy_z(t).wait_recv()
            act = jnp.maximum(kept[t] + zrecv[t] + b[:, at], 0.0) * w2[:, at]
            total = jnp.sum(act, axis=1, keepdims=True)
            fsend[...] = fsend[...] + jnp.where(spots == trace_of(k), total, 0.0)

    pl.semaphore_wait(far, 1)
    pltpu.make_async_copy(wown, wown, s_win.at[chunks]).wait()

    def run(order, lag, ahead, ends):
        arrived = set()
        for kind, k, c in schedule(order, blocks, lag, ahead):
            if kind == 0:
                for p in range(PARTS):
                    collect(k * PARTS + p, ends)
            elif kind == 1:
                ready(k)
            else:
                if c not in arrived:
                    arrived.add(c)
                    copy_w(c).wait_recv()
                (give if kind == 2 else take)(k, c)

    @pl.when(is_end)
    def _():
        run(row_order(blocks, chunks), END_LAG, END_AHEAD, True)

    @pl.when(middle)
    def _():
        run(wave_order(blocks, chunks), MID_LAG, MID_AHEAD, False)

    for k in range(blocks):
        for j in range(chunks // 2):
            finish(k, j)

    me = s * n_head + h
    n_dev = n_seq * n_head

    def copy_f(d):
        to = lax.rem(me + d, n_dev)
        return remote(
            frecv.at[me], frecv.at[me], s_f, r_f, to // n_head, lax.rem(to, n_head)
        )

    frecv[me] = jnp.transpose(fsend[...])[: frecv.shape[1], :]
    for d in range(1, n_dev):
        copy_f(d).start()
    def drain(ref, sem):
        remote(ref, ref, sem, r_f, across, h).wait_send()

    drain(wown, s_w)
    drain(xin, s_x1)
    drain(xin, s_x2)
    drain(xin, s_x3.at[0])

    @pl.when(member)
    def _():
        drain(xin, s_x3.at[1])

    drain(ysend, s_y)
    left = h < n_head // 2
    for side in range(2):
        for up in range(2):
            sent = sum(
                up != owner_of(k, j)[side] for k in range(blocks) for j in range(chunks // 2)
            )

            @pl.when((left == (side == 0)) & (high == up))
            def _():
                drain(zsend.at[pl.ds(0, sent)], s_z)

    others = frecv.at[pl.ds(0, n_dev - 1)]
    remote(others, others, s_f, r_f, across, h).wait_recv()

    sums = [frecv[i] for i in range(4)]
    for i in range(4, n_dev):
        sums[i % 4] = sums[i % 4] + frecv[i]
    logit = (sums[0] + sums[1]) + (sums[2] + sums[3])

    live = valid[...] == 1
    low = jnp.min(jnp.where(live, logit, 1e30), axis=1, keepdims=True)
    ids = lax.broadcasted_iota(jnp.int32, (traces, pairs.shape[1]), 0)
    square = (pairs.shape[1], pairs.shape[1])
    eye = lax.broadcasted_iota(jnp.int32, square, 0) == lax.broadcasted_iota(jnp.int32, square, 1)
    winner = jnp.sum(jnp.where(pairs[0:1, :] == ids, low, 0.0), axis=0, keepdims=True)
    loser = jnp.sum(jnp.where(pairs[1:2, :] == ids, low, 0.0), axis=0, keepdims=True)
    gap = jnp.sum(jnp.where(eye, winner - loser, 0.0), axis=1, keepdims=True)
    result[:traces, :steps] = jnp.where(live, logit, 0.0)
    result[:traces, steps : steps + 1] = low
    result[: pairs.shape[1], steps + 1 : steps + 2] = gap

    drain(others, s_f)


def fused(n_seq, n_head, hidden_states, boundary, valid, pairs, w_first, b_first, w_second):
    traces, toks, feats = hidden_states.shape
    steps = boundary.shape[1]
    depth, width = w_first.shape
    block, cols = steps // 2, width // 2
    chunks = cols // SPAN
    mine = traces * chunks // 2
    pieces = traces * PARTS
    n_dev = n_seq * n_head
    bf16, f32 = jnp.bfloat16, jnp.float32
    dma = pltpu.SemaphoreType.DMA
    vmem = pl.BlockSpec(memory_space=pltpu.VMEM)
    hbm = pl.BlockSpec(memory_space=pl.ANY)
    result = pl.pallas_call(
        functools.partial(kernel, n_seq, n_head),
        out_shape=jax.ShapeDtypeStruct((max(traces, pairs.shape[0]), steps + 64), f32),
        in_specs=[hbm] + [vmem] * 3 + [hbm] + [vmem] * 2,
        out_specs=vmem,
        scratch_shapes=[
            pltpu.VMEM((traces, toks, feats), bf16),
            pltpu.VMEM((2, traces, block, feats), bf16),
            pltpu.VMEM((traces, block, feats), bf16),
            pltpu.VMEM((traces, block, feats), bf16),
            pltpu.VMEM((traces, block, feats), bf16),
            pltpu.VMEM((2, traces, block, feats), bf16),
            pltpu.VMEM((traces, steps, feats), bf16),
            pltpu.VMEM((chunks, depth, SPAN), bf16),
            pltpu.VMEM((chunks, 2 * depth, SPAN), bf16),
            pltpu.VMEM((mine, steps, SPAN), f32),
            pltpu.VMEM((mine, steps, SPAN), f32),
            pltpu.VMEM((mine, steps, SPAN), f32),
            pltpu.VMEM((mine, steps, SPAN), f32),
            pltpu.VMEM((mine, steps, SPAN), f32),
            pltpu.VMEM((steps, 128), f32),
            pltpu.VMEM((n_dev, traces, steps), f32),
            pltpu.SemaphoreType.REGULAR,
            dma((traces,)), dma((chunks + 1,)),
            dma, dma((pieces,)),
            dma, dma((chunks,)),
            dma, dma((pieces,)), dma((pieces,)),
            dma((2,)), dma((pieces + traces,)),
            dma, dma((mine,)),
            dma, dma((mine,)),
            dma, dma,
        ],
        compiler_params=pltpu.CompilerParams(collective_id=0, has_side_effects=True),
    )(
        hidden_states, boundary, valid, pairs.T, w_first,
        b_first.reshape(1, width), w_second.reshape(1, width),
    )
    return result[:traces, :steps], result[:traces, steps], result[: pairs.shape[0], steps + 1]


def solution(mesh):
    n_seq, n_head = mesh.shape["seq"], mesh.shape["head"]
    paired = n_seq == 8 and n_head == 4
    body = functools.partial(fused, n_seq, n_head) if paired else per_device
    placed = (P(None, "seq", "head"), P(), P(), P(), P("seq", "head"), P("head"), P("head"))
    return jax.shard_map(
        body, mesh=mesh, in_specs=placed, out_specs=(P(), P(), P()), check_vma=False
    )
```
